32 devices in a mesh: gx: 4 (over z), gy: 4 (over y, core), gz: 2 (over x).
Axes of the slice: x: 2, y: 2, z: 4, core: 2. Of those that a mesh axis runs over, the one named last changes fastest.
Arguments:
- gas_position: float32 [3, 131072], P(None, ('gx', 'gy', 'gz')), may hold values from 0 to 1
- gas_mass: float32 [131072], P(('gx', 'gy', 'gz')), may hold values from 0.3 to 3
- gas_smoothing: float32 [131072], P(('gx', 'gy', 'gz')), may hold values from 0.5 to 1.5
- leaf_counts: int32 [1024], P(('gx', 'gy', 'gz')), may hold values from 64 to 128
- ghost_lists: int32 [32, 4, 2], P(('gx', 'gy', 'gz')), may hold values from 0 to 31, as said below
- star_position: float32 [3, 65536], P(None, ('gx', 'gy', 'gz')), may hold values from 0 to 1
- star_energy: float32 [65536], P(('gx', 'gy', 'gz')), may hold values from 0.1 to 10
- star_momentum: float32 [3, 65536], P(None, ('gx', 'gy', 'gz')), may hold values from -6 to 6
- block_counts: int32 [512], P(('gx', 'gy', 'gz')), may hold values from 1 to 128
- block_owners: int32 [512, 1], P(('gx', 'gy', 'gz')), may hold values from 0 to 7; in each aligned block of 16 rows (0 to 15, 16 to 31, ...) at most 3 rows name the same one
- block_leaves: int32 [512], P(('gx', 'gy', 'gz')), may hold values from 0 to 31
Outputs:
- accel: float32 [3, 131072], P(None, ('gx', 'gy', 'gz'))
- deposit: float32 [4, 131072], P(None, ('gx', 'gy', 'gz'))
The draws below stay inside these ranges and needn't reach their ends.
Inputs may be any that keep to these rules, and one draw needn't show every extreme that they name: `ghost_lists`: each of the four lists of a device names 2 different leaves. `block_owners`: among the 16 star blocks of one device, no owner is named more than 3 times, and in some devices one owner is named exactly 3 times.
All inputs are finite; a program needn't handle non-finite values.
Results may differ from the reference program's by a relative error of at most 0.00015.
Values sent between devices are 32-bit elements; how exact they have to be, the bound alone decides.
A program may use at most 64 MiB of HBM per device.

```python
import math
import jax
import jax.numpy as jnp
import numpy as np
from jax import lax

LEAVES = 32
LEAF_SLOTS = 128
GHOSTS = 2
STARS_BLOCK = 128
SLOTS = 3
OWNERS = 8
BLOCKS = 16
PARTICLES = 131072
STAR_BLOCKS = 512
STARS = 65536
N_GX = 4
N_GY = 4
N_GZ = 2
DEVICES = 32


def draw_ghost_lists(key, part):
    keys = jax.random.split(jax.random.fold_in(key, 17), DEVICES * 4)
    picks = jax.vmap(lambda one_key: jax.random.permutation(one_key, LEAVES)[:GHOSTS])(keys)
    return picks.reshape(DEVICES, 4, GHOSTS).astype(jnp.int32)


def set_ends(values, rng, least, high):
    dims = values.shape
    place = [jax.random.randint(jax.random.fold_in(rng, axis), (), 0, dims[axis]) for axis in range(len(dims))]
    values = values.at[tuple(place)].set(least)
    longest = dims.index(max(dims))
    place[longest] = (place[longest] + 1) % dims[longest]
    return values.at[tuple(place)].set(high)


def levels(key, dims, cuts, low, high):
    factor_of, own = 1.0, jax.random.fold_in(key, 6)
    for dim, parts in cuts:
        draws = jnp.exp(jax.random.uniform(jax.random.fold_in(own, dim), (parts,), jnp.float32, low / len(cuts), high / len(cuts)))
        factor_of = factor_of * jnp.repeat(draws, dims[dim] // parts).reshape([-1 if axis == dim else 1 for axis in range(len(dims))])
    return factor_of


def assign_block(stream_key, own, number, rows, count, top, reach, lean):
    ranking = jax.random.permutation(stream_key, count)
    heavy_load, ordinary = portions_of(count, rows * top, reach, lean, True), portions_of(count, rows * top, reach, lean, False)
    places = jnp.arange(count)

    def named(sizes, turn):
        used = int((sizes > 0).sum())
        fixed = max(1, used // 4)
        shifted = fixed + (places - fixed + turn * (used - fixed)) % max(1, count - fixed)
        return jnp.zeros((count,), jnp.int32).at[ranking[jnp.where(places < fixed, places, shifted)]].set(jnp.asarray(sizes, jnp.int32))

    sizes = jnp.where(number % 4 == 0, named(heavy_load, number // 4), named(ordinary, number - number // 4 - 1))
    mixed = jax.random.permutation(jax.random.fold_in(own, 3), count)
    giver, receiver = mixed[0:count // 2 * 2:2], mixed[1:count // 2 * 2:2]
    room = jnp.minimum(sizes[giver] - 1, reach - sizes[receiver]) // 2
    room = jnp.where((giver == ranking[0]) | (receiver == ranking[0]) | (sizes[receiver] == 0), 0, jnp.maximum(room, 0))
    shifted = jax.random.randint(jax.random.fold_in(own, 4), (count // 2,), 0, 1 << 20) % (room + 1)
    sizes = sizes.at[giver].add(-shifted).at[receiver].add(shifted)
    members = jnp.searchsorted(jnp.cumsum(sizes), jnp.arange(rows * top), side="right").astype(jnp.int32)
    table = members.reshape(top, rows).T
    table = table[jax.random.permutation(jax.random.fold_in(own, 1), rows)]
    turn = jax.random.randint(jax.random.fold_in(own, 2), (rows, 1), 0, top)
    return jnp.take_along_axis(table, (jnp.arange(top)[None, :] + turn) % top, axis=1)


def portions_of(count, total, reach, lean, full):
    weights = [(1 << 20) // math.isqrt(rank ** lean) + 1 for rank in range(1, count + 1)]
    largest = reach if full else min(reach, max(-(-total // count), total * weights[0] // sum(weights)))
    least = 1 if total - largest >= count - 1 else 0
    counts, spare = [largest] + [least] * (count - 1), total - largest - least * (count - 1)
    while spare > 0:
        movable = [i for i in range(1, count) if counts[i] < largest] or [i for i in range(1, count) if counts[i] < reach]
        whole, budget = sum([weights[i] for i in movable]), spare
        for i in movable:
            addition = min(reach - counts[i], max(1, budget * weights[i] // whole), spare)
            counts[i] = counts[i] + addition
            spare = spare - addition
    return np.array(counts)


def gaussian(own_key, dims, scale, limit, cuts=(), kind=jnp.bfloat16):
    gain = levels(own_key, dims, cuts, -0.22, 0.18) if cuts else 1.0
    entries = jax.random.normal(own_key, dims, jnp.float32) * scale * gain
    return jnp.minimum(jnp.maximum(entries, -limit), limit).astype(kind)


def setup_inputs(seed: int = 0) -> dict:
    streams_of = jax.random.split(jax.random.key(seed), 12)
    gas_position = jnp.clip(1.0 * jax.random.uniform(streams_of[0], (3, PARTICLES), jnp.float32) ** levels(streams_of[0], (3, PARTICLES), ((1, 32),), -0.2, 0.2), 0.0, 1.0)
    gas_mass = jnp.clip(jnp.exp(math.log(3.0) - 2.3025851 * jax.random.uniform(streams_of[1], (PARTICLES,), jnp.float32) ** levels(streams_of[1], (PARTICLES,), ((0, 32),), -0.2, 0.2)), 0.3, 3.0)
    gas_smoothing = jnp.clip(jnp.exp(math.log(1.5) - 1.0986123 * jax.random.uniform(streams_of[2], (PARTICLES,), jnp.float32) ** levels(streams_of[2], (PARTICLES,), ((0, 32),), -0.2, 0.2)), 0.5, 1.5)
    leaf_counts = set_ends(jax.random.randint(streams_of[3], (DEVICES * LEAVES,), LEAF_SLOTS // 2, LEAF_SLOTS + 1), jax.random.fold_in(streams_of[3], 1), LEAF_SLOTS // 2, LEAF_SLOTS).astype(jnp.int32)
    ghost_lists = draw_ghost_lists(jax.random.fold_in(streams_of[11], 71), 0)
    star_position = jnp.clip(1.0 * jax.random.uniform(streams_of[5], (3, STARS), jnp.float32) ** levels(streams_of[5], (3, STARS), ((1, 32),), -0.2, 0.2), 0.0, 1.0)
    star_energy = jnp.clip(jnp.exp(math.log(10.0) - 4.6051702 * jax.random.uniform(streams_of[6], (STARS,), jnp.float32) ** levels(streams_of[6], (STARS,), ((0, 32),), -0.2, 0.2)), 0.1, 10.0)
    star_momentum = gaussian(streams_of[7], (3, STARS), 1.0, 6.0, ((1, 32),), jnp.float32)
    block_counts = set_ends(jax.random.randint(streams_of[8], (STAR_BLOCKS,), 1, STARS_BLOCK + 1), jax.random.fold_in(streams_of[8], 1), 1, STARS_BLOCK).astype(jnp.int32)
    block_owners_keys = jax.random.split(jax.random.fold_in(streams_of[9], 1), STAR_BLOCKS // BLOCKS)
    block_owners_turns = jax.random.permutation(jax.random.fold_in(streams_of[9], 3), STAR_BLOCKS // BLOCKS)
    block_owners = jax.vmap(lambda own, number: assign_block(jax.random.fold_in(streams_of[9], 2), own, number, BLOCKS, OWNERS, 1, SLOTS, 2))(block_owners_keys, block_owners_turns).reshape((STAR_BLOCKS, 1))
    block_leaves = set_ends(jax.random.randint(streams_of[10], (STAR_BLOCKS,), 0, LEAVES), jax.random.fold_in(streams_of[10], 1), 0, LEAVES - 1).astype(jnp.int32)
    return {"gas_position": gas_position, "gas_mass": gas_mass, "gas_smoothing": gas_smoothing, "leaf_counts": leaf_counts, "ghost_lists": ghost_lists, "star_position": star_position, "star_energy": star_energy, "star_momentum": star_momentum, "block_counts": block_counts, "block_owners": block_owners, "block_leaves": block_leaves}


SPLIT_SQ = 1.0
SOFT_SQ = 0.01
GRAVITY = 0.002
RADIAL_PUSH = 1.0

def pair_accel(targets, sources, source_mass):
    sep_x = sources[0][None, :] - targets[0][:, None]
    sep_y = sources[1][None, :] - targets[1][:, None]
    sep_z = sources[2][None, :] - targets[2][:, None]
    distance = sep_x * sep_x + sep_y * sep_y + sep_z * sep_z
    soften = distance + SOFT_SQ
    kernel = source_mass[None, :] * jnp.exp(-distance / SPLIT_SQ) / (soften * jnp.sqrt(soften))
    return GRAVITY * jnp.stack([lax.optimization_barrier(jnp.sum(sep_x * kernel, axis=1)), lax.optimization_barrier(jnp.sum(sep_y * kernel, axis=1)), lax.optimization_barrier(jnp.sum(sep_z * kernel, axis=1))])

def deposit_block(star_xyz, energy_in, momentum_in, gas_xyz, inverse):
    seps = [gas_xyz[axis_num][None, :] - star_xyz[axis_num][:, None] for axis_num in range(3)]
    distance = seps[0] * seps[0] + seps[1] * seps[1] + seps[2] * seps[2]
    weight = jnp.exp(-distance * inverse[None, :])
    normaliser = 1.0 + lax.optimization_barrier(jnp.sum(weight, axis=1))
    shares = weight / normaliser[:, None]
    heated = lax.optimization_barrier(jnp.sum(energy_in[:, None] * shares, axis=0))
    kicks = [lax.optimization_barrier(jnp.sum(shares * (momentum_in[axis_num][:, None] + RADIAL_PUSH * energy_in[:, None] * seps[axis_num]), axis=0)) for axis_num in range(3)]
    return jnp.stack([heated] + kicks)

def reference(gas_position, gas_mass, gas_smoothing, leaf_counts, ghost_lists, star_position, star_energy, star_momentum, block_counts, block_owners, block_leaves):
    grid = (N_GX, N_GY, N_GZ)
    slot_iota = jnp.arange(LEAF_SLOTS, dtype=jnp.int32)
    alive = slot_iota < leaf_counts.reshape(grid + (LEAVES, 1))
    masses = jnp.where(alive, gas_mass.reshape(grid + (LEAVES, LEAF_SLOTS)), jnp.float32(0.0))
    carried = jnp.concatenate([gas_position.reshape((3,) + grid + (LEAVES, LEAF_SLOTS)), masses[None]], axis=0)
    chosen_all = ghost_lists.reshape(grid + (4, GHOSTS))

    def select_ghosts(which):
        chosen = jnp.broadcast_to(chosen_all[None, :, :, :, which, :, None], (4,) + grid + (GHOSTS, LEAF_SLOTS))
        return jnp.take_along_axis(carried, chosen, axis=4)
    arrivals = []
    for which, shift_by, grid_axis, component, offset in ((0, 1, 1, 0, -1.0), (1, -1, 1, 0, 1.0), (2, 1, 2, 1, -1.0), (3, -1, 2, 1, 1.0)):
        moved = jnp.roll(select_ghosts(which), shift_by, axis=grid_axis)
        moved = moved.at[component].add(offset)
        arrivals.append(moved.reshape(4, DEVICES, GHOSTS * LEAF_SLOTS))
    sources = jnp.concatenate([carried.reshape(4, DEVICES, LEAVES * LEAF_SLOTS)] + arrivals, axis=2).transpose(1, 0, 2)
    targets = gas_position.reshape(3, DEVICES, LEAVES * LEAF_SLOTS).transpose(1, 0, 2)
    accel_all = lax.map(lambda pair_items: pair_accel(pair_items[0], pair_items[1][:3], pair_items[1][3]), (targets, sources))
    alive_flat = alive.reshape(PARTICLES)
    accel = jnp.where(alive_flat[None, :], accel_all.transpose(1, 0, 2).reshape(3, PARTICLES), jnp.float32(0.0))
    star_live = jnp.arange(STARS_BLOCK, dtype=jnp.int32)[None, :] < block_counts[:, None]
    star_xyz = star_position.reshape(3, STAR_BLOCKS, STARS_BLOCK).transpose(1, 0, 2)
    energy_in = jnp.where(star_live, star_energy.reshape(STAR_BLOCKS, STARS_BLOCK), jnp.float32(0.0))
    momentum_in = jnp.where(star_live[:, None, :], star_momentum.reshape(3, STAR_BLOCKS, STARS_BLOCK).transpose(1, 0, 2), jnp.float32(0.0))
    source_dev = jnp.arange(STAR_BLOCKS, dtype=jnp.int32) // BLOCKS
    dest_dev = source_dev // OWNERS * OWNERS + block_owners[:, 0].astype(jnp.int32)
    gas_leaf = (dest_dev * LEAVES + block_leaves).astype(jnp.int32)
    gas_xyz = gas_position.reshape(3, DEVICES * LEAVES, LEAF_SLOTS).transpose(1, 0, 2)
    inverse = (1.0 / (gas_smoothing * gas_smoothing)).reshape(DEVICES * LEAVES, LEAF_SLOTS)

    def one_block(items):
        xyz, energy_one, momentum_one, leaf_id = items
        return deposit_block(xyz, energy_one, momentum_one, gas_xyz[leaf_id], inverse[leaf_id])
    per_block = lax.map(one_block, (star_xyz, energy_in, momentum_in, gas_leaf), batch_size=64)
    totals = jax.ops.segment_sum(per_block, gas_leaf, num_segments=DEVICES * LEAVES)
    deposit = jnp.where(alive_flat[None, :], totals.transpose(1, 0, 2).reshape(4, PARTICLES), jnp.float32(0.0))
    return (accel, deposit)
```

```python
import functools
import math

import jax
import jax.numpy as jnp
from jax import lax
from jax.experimental import pallas as pl
from jax.experimental.pallas import tpu as pltpu
from jax.sharding import PartitionSpec as P

LANES = 128
SLOTS = 3
SPLIT_SQ = 1.0
SOFT_SQ = 0.01
GRAVITY = 0.002
RADIAL_PUSH = 1.0

SCALE = math.log2(math.e) / (1.5 * SPLIT_SQ)
FACTOR = GRAVITY * math.exp(SOFT_SQ / SPLIT_SQ) * SCALE**1.5
FEATURES = 40
MESH = pl.DeviceIdType.MESH
HIGHEST = lax.Precision.HIGHEST
F32 = jnp.float32
BF16 = jnp.bfloat16

TARGETS = 512
SOURCES = 256
UNROLL = 4


def split3(x):
    a = x.astype(BF16).astype(F32)
    rest = x - a
    b = rest.astype(BF16).astype(F32)
    return a, b, rest - b


def prepare_sends(
    sizes,
    pos_ref, mass_ref, count_ref, ghost_ref,
    star_pos_ref, energy_ref, star_mom_ref, block_count_ref, owner_ref, leaf_ref,
    src, ghost_send, star_send,
):
    n_x, n_y, n_z, leaves, ghosts, blocks = sizes
    owners = n_y * n_z
    rows = leaves * LANES
    lane = lax.broadcasted_iota(jnp.int32, (1, LANES), 1)

    src[0:3, :] = pos_ref[...]
    src[4:8, :] = jnp.zeros((4, rows), F32)
    for l in range(leaves):
        here = slice(l * LANES, (l + 1) * LANES)
        alive = lane < count_ref[l]
        src[3:4, here] = jnp.where(alive, mass_ref[l : l + 1, :], 0.0)
        src[4:5, here] = jnp.where(alive, 1.0, 0.0).astype(F32)
    for k in range(4):
        for g in range(ghosts):
            start = pl.multiple_of(ghost_ref[k * ghosts + g] * LANES, LANES)
            ghost_send[k, :, g * LANES : (g + 1) * LANES] = src[:, pl.ds(start, LANES)]

    @pl.loop(0, owners)
    def _(o):
        def scan(b, found):
            hit = owner_ref[b] == o
            i0, i1, i2 = found
            return (jnp.where(hit, b, i0), jnp.where(hit, i0, i1), jnp.where(hit, i1, i2))

        none = jnp.int32(-1)
        found = lax.fori_loop(0, blocks, scan, (none,) * SLOTS, unroll=8)
        for k in range(SLOTS):
            b = jnp.maximum(found[k], 0)
            valid = found[k] >= 0
            start = pl.multiple_of(b * LANES, LANES)
            live = lane < jnp.where(valid, block_count_ref[b], 0)
            named = lane == jnp.where(valid, leaf_ref[b], -1)
            star_send[o, k, 0:3] = star_pos_ref[:, pl.ds(start, LANES)]
            star_send[o, k, 3:4] = jnp.where(live, energy_ref[pl.ds(b, 1), :], 0.0)
            star_send[o, k, 4:7] = jnp.where(live, star_mom_ref[:, pl.ds(start, LANES)], 0.0)
            star_send[o, k, 7:8] = jnp.where(named, 1.0, 0.0).astype(F32)


def kernel(
    sizes,
    own_ref, smooth_ref, ghost_send, star_send,
    accel_ref, deposit_ref,
    src, ghost_recv, star_recv,
    feat, side_a, side_b, weights, acc, table, marker, gathered, dep,
    ghost_ssem, ghost_rsem, star_ssem, star_rsem,
):
    n_x, n_y, n_z, leaves, ghosts, blocks = sizes
    owners = n_y * n_z
    rows = leaves * LANES
    wide = ghosts * LANES
    x, y, z = lax.axis_index("gx"), lax.axis_index("gy"), lax.axis_index("gz")
    me = y * n_z + z

    def owner_at(d):
        other = lax.rem(me + d, owners)
        return other, (x, lax.div(other, n_z), lax.rem(other, n_z))

    def beside(k):
        step = 1 if k % 2 == 0 else -1
        if k < 2:
            return (lax.rem(x + step + n_x, n_x), y, z)
        return (x, lax.rem(y + step + n_y, n_y), z)

    barrier = pltpu.get_barrier_semaphore()
    for k in range(2):
        pl.semaphore_signal(barrier, inc=1, device_id=beside(k), device_id_type=MESH)

    @pl.loop(1, owners)
    def _(d):
        pl.semaphore_signal(barrier, inc=1, device_id=owner_at(d)[1], device_id_type=MESH)

    src[:, 0:rows] = own_ref[...]
    pl.semaphore_wait(barrier, owners + 1)

    def ghost_copy(k):
        return pltpu.make_async_remote_copy(
            src_ref=ghost_send.at[k], dst_ref=ghost_recv.at[k],
            send_sem=ghost_ssem.at[k], recv_sem=ghost_rsem.at[k],
            device_id=beside(k), device_id_type=MESH,
        )

    def star_copy(d):
        other, where = owner_at(d)
        return pltpu.make_async_remote_copy(
            src_ref=star_send.at[other], dst_ref=star_recv.at[me],
            send_sem=star_ssem.at[d], recv_sem=star_rsem.at[d],
            device_id=where, device_id_type=MESH,
        )

    for k in range(4):
        ghost_copy(k).start()

    @pl.loop(1, owners)
    def _(d):
        star_copy(d).start()

    star_recv[me] = star_send[me]

    def put(rows_of):
        at = 0
        for piece in rows_of:
            feat[at : at + piece.shape[0], :] = piece
            at += piece.shape[0]
        if at < FEATURES:
            feat[at:FEATURES, :] = jnp.zeros((FEATURES - at, SOURCES), F32)

    def prepare(start, targets):
        here = pl.ds(start, SOURCES)
        u = src[0:3, here] - 0.5
        mass = src[3:4, here]
        norm = SCALE * jnp.sum(u * u, axis=0, keepdims=True)
        a = split3((-2.0 * SCALE) * u)
        n = split3(norm + SCALE * SOFT_SQ)
        one = jnp.ones((1, SOURCES), F32)
        put([a[0]] * 3 + [a[1]] * 3 + [a[2]] * 3 + list(n) + [one] * 3)
        side_a[here, :] = feat[...].T.astype(BF16)
        wx, wm = split3(mass * u), split3(mass)
        put([wx[0], wm[0], wx[1], wm[1], wx[2], wm[2]])
        weights[:, here] = feat[0:16, :].astype(BF16)
        if targets:
            b = split3(u)
            put(list(b) * 3 + [one] * 3 + list(split3(norm)))
            side_b[:, here] = feat[...].astype(BF16)

    @pl.loop(0, rows // SOURCES)
    def _(c):
        prepare(pl.multiple_of(c * SOURCES, SOURCES), True)

    def pairs(start, right):
        d = jnp.dot(
            side_a[pl.ds(start, SOURCES), :], right, preferred_element_type=F32
        )
        value = jnp.exp2(-1.5 * (d + lax.log2(d)))
        high = value.astype(BF16)
        low = (value - high.astype(F32)).astype(BF16)
        w = weights[:, pl.ds(start, SOURCES)]
        return jnp.dot(w, high, preferred_element_type=F32) + jnp.dot(
            w, low, preferred_element_type=F32
        )

    def over(first, count, right, total, unroll):
        def step(c, total):
            start = pl.multiple_of(first + c * SOURCES, SOURCES)
            return total + pairs(start, right)

        return lax.fori_loop(0, count, step, total, unroll=unroll)

    @pl.loop(0, rows // TARGETS)
    def _(t):
        here = pl.ds(pl.multiple_of(t * TARGETS, TARGETS), TARGETS)
        acc[:, here] = over(
            0, rows // SOURCES, side_b[:, here], jnp.zeros((16, TARGETS), F32), UNROLL
        )

    for k in range(4):
        ghost_copy(k).wait()
        there = slice(rows + k * wide, rows + (k + 1) * wide)
        src[:, there] = ghost_recv[k]
        shifted = slice(k // 2, k // 2 + 1)
        src[shifted, there] = src[shifted, there] + (-1.0 if k % 2 == 0 else 1.0)

    @pl.loop(0, 4 * wide // SOURCES)
    def _(c):
        prepare(pl.multiple_of(rows + c * SOURCES, SOURCES), False)

    @pl.loop(0, rows // TARGETS)
    def _(t):
        here = pl.ds(pl.multiple_of(t * TARGETS, TARGETS), TARGETS)
        total = over(rows, 4 * wide // SOURCES, side_b[:, here], acc[:, here], True)
        total = total[0:4] + total[4:8] + total[8:12]
        u = src[0:3, here] - 0.5
        value = FACTOR * (total[0:3] - u * total[3:4])
        accel_ref[:, here] = jnp.where(src[4:5, here] > 0.5, value, 0.0)

    h = smooth_ref[...]
    table[:, 3 * LANES :] = 1.0 / (h * h)
    for l in range(leaves):
        for c in range(3):
            table[l : l + 1, c * LANES : (c + 1) * LANES] = src[
                c : c + 1, l * LANES : (l + 1) * LANES
            ]

    @pl.loop(1, owners)
    def _(d):
        star_copy(d).wait()

    @pl.loop(0, owners)
    def _(o):
        for k in range(SLOTS):
            marker[pl.ds(o * SLOTS + k, 1), :] = star_recv[o, k, 7:8]

    for c in range(4):
        gathered[c] = jnp.dot(
            marker[:, 0:leaves],
            table[:, c * LANES : (c + 1) * LANES],
            precision=HIGHEST,
            preferred_element_type=F32,
        )

    @pl.loop(0, owners)
    def _(o):
        for k in range(SLOTS):
            at = pl.ds(o * SLOTS + k, 1)
            star = star_recv[o, k].T
            gas = [gathered[c, at, :] for c in range(4)]
            seps = [gas[c] - star[:, c : c + 1] for c in range(3)]
            distance = seps[0] * seps[0] + seps[1] * seps[1] + seps[2] * seps[2]
            weight = jnp.exp(-distance * gas[3])
            share = weight / (1.0 + jnp.sum(weight, axis=1, keepdims=True))
            heat = star[:, 3:4] * share
            dep[0, at, :] = jnp.sum(heat, axis=0, keepdims=True)
            for c in range(3):
                kick = share * star[:, 4 + c : 5 + c] + RADIAL_PUSH * heat * seps[c]
                dep[c + 1, at, :] = jnp.sum(kick, axis=0, keepdims=True)

    named = marker[...].T[0:leaves]
    for c in range(4):
        table[:, c * LANES : (c + 1) * LANES] = jnp.dot(
            named, dep[c], precision=HIGHEST, preferred_element_type=F32
        )
    for l in range(leaves):
        alive = src[4:5, l * LANES : (l + 1) * LANES] > 0.5
        for c in range(4):
            deposit_ref[c : c + 1, l * LANES : (l + 1) * LANES] = jnp.where(
                alive, table[l : l + 1, c * LANES : (c + 1) * LANES], 0.0
            )


def on_device(
    mesh_sizes,
    gas_position, gas_mass, gas_smoothing, leaf_counts, ghost_lists,
    star_position, star_energy, star_momentum, block_counts, block_owners, block_leaves,
):
    n_x, n_y, n_z = mesh_sizes
    leaves = leaf_counts.shape[0]
    blocks = block_counts.shape[0]
    ghosts = ghost_lists.shape[2]
    rows = leaves * LANES
    owners = n_y * n_z
    slots = owners * SLOTS
    slot_rows = -(-slots // 8) * 8
    total = rows + 4 * ghosts * LANES
    vmem = pl.BlockSpec(memory_space=pltpu.VMEM)
    smem = pl.BlockSpec(memory_space=pltpu.SMEM)
    sizes = (n_x, n_y, n_z, leaves, ghosts, blocks)
    own, ghost_send, star_send = pl.pallas_call(
        functools.partial(prepare_sends, sizes),
        out_shape=(
            jax.ShapeDtypeStruct((8, rows), F32),
            jax.ShapeDtypeStruct((4, 8, ghosts * LANES), F32),
            jax.ShapeDtypeStruct((owners, SLOTS, 8, LANES), F32),
        ),
        in_specs=[vmem, vmem, smem, smem, vmem, vmem, vmem, smem, smem, smem],
        out_specs=(vmem, vmem, vmem),
    )(
        gas_position,
        gas_mass.reshape(leaves, LANES),
        leaf_counts,
        ghost_lists.reshape(-1),
        star_position,
        star_energy.reshape(blocks, LANES),
        star_momentum,
        block_counts,
        block_owners.reshape(-1),
        block_leaves,
    )
    return pl.pallas_call(
        functools.partial(kernel, sizes),
        out_shape=(
            jax.ShapeDtypeStruct((3, rows), F32),
            jax.ShapeDtypeStruct((4, rows), F32),
        ),
        in_specs=[vmem, vmem, vmem, vmem],
        out_specs=(vmem, vmem),
        scratch_shapes=[
            pltpu.VMEM((8, total), F32),
            pltpu.VMEM((4, 8, ghosts * LANES), F32),
            pltpu.VMEM((owners, SLOTS, 8, LANES), F32),
            pltpu.VMEM((FEATURES, SOURCES), F32),
            pltpu.VMEM((total, FEATURES), BF16),
            pltpu.VMEM((FEATURES, rows), BF16),
            pltpu.VMEM((16, total), BF16),
            pltpu.VMEM((16, rows), F32),
            pltpu.VMEM((leaves, 4 * LANES), F32),
            pltpu.VMEM((slot_rows, LANES), F32),
            pltpu.VMEM((4, slot_rows, LANES), F32),
            pltpu.VMEM((4, slot_rows, LANES), F32),
            pltpu.SemaphoreType.DMA((4,)),
            pltpu.SemaphoreType.DMA((4,)),
            pltpu.SemaphoreType.DMA((owners,)),
            pltpu.SemaphoreType.DMA((owners,)),
        ],
        compiler_params=pltpu.CompilerParams(collective_id=0, has_side_effects=True),
    )(own, gas_smoothing.reshape(leaves, LANES), ghost_send, star_send)


def solution(mesh):
    split = ("gx", "gy", "gz")
    placed = (
        P(None, split), P(split), P(split), P(split), P(split, None, None),
        P(None, split), P(split), P(None, split), P(split), P(split, None), P(split),
    )
    sizes = tuple(mesh.shape[axis] for axis in split)
    return jax.shard_map(
        functools.partial(on_device, sizes),
        mesh=mesh,
        in_specs=placed,
        out_specs=(P(None, split), P(None, split)),
        check_vma=False,
    )
```

```python
import functools
import math

import jax
import jax.numpy as jnp
from jax import lax
from jax.experimental import pallas as pl
from jax.experimental.pallas import tpu as pltpu
from jax.sharding import PartitionSpec as P

LANES = 128
SLOTS = 3
SPLIT_SQ = 1.0
SOFT_SQ = 0.01
GRAVITY = 0.002
RADIAL_PUSH = 1.0

SCALE = math.log2(math.e) / (1.5 * SPLIT_SQ)
FACTOR = GRAVITY * math.exp(SOFT_SQ / SPLIT_SQ) * SCALE**1.5
FEATURES = 40
MESH = pl.DeviceIdType.MESH
HIGHEST = lax.Precision.HIGHEST
F32 = jnp.float32
BF16 = jnp.bfloat16

TARGETS = 1024
SOURCES = 256
UNROLL = 2


def split3(x):
    a = x.astype(BF16).astype(F32)
    rest = x - a
    b = rest.astype(BF16).astype(F32)
    return a, b, rest - b


def prepare_sends(
    sizes,
    pos_ref, mass_ref, count_ref, ghost_ref,
    star_pos_ref, energy_ref, star_mom_ref, block_count_ref, owner_ref, leaf_ref,
    src, ghost_send, star_send,
):
    n_x, n_y, n_z, leaves, ghosts, blocks = sizes
    owners = n_y * n_z
    rows = leaves * LANES
    lane = lax.broadcasted_iota(jnp.int32, (1, LANES), 1)

    src[0:3, :] = pos_ref[...]
    src[4:8, :] = jnp.zeros((4, rows), F32)
    for l in range(leaves):
        here = slice(l * LANES, (l + 1) * LANES)
        alive = lane < count_ref[l]
        src[3:4, here] = jnp.where(alive, mass_ref[l : l + 1, :], 0.0)
        src[4:5, here] = jnp.where(alive, 1.0, 0.0).astype(F32)
    for k in range(4):
        for g in range(ghosts):
            start = pl.multiple_of(ghost_ref[k * ghosts + g] * LANES, LANES)
            ghost_send[k, :, g * LANES : (g + 1) * LANES] = src[:, pl.ds(start, LANES)]

    @pl.loop(0, owners)
    def _(o):
        def scan(b, found):
            hit = owner_ref[b] == o
            i0, i1, i2 = found
            return (jnp.where(hit, b, i0), jnp.where(hit, i0, i1), jnp.where(hit, i1, i2))

        none = jnp.int32(-1)
        found = lax.fori_loop(0, blocks, scan, (none,) * SLOTS, unroll=8)
        for k in range(SLOTS):
            b = jnp.maximum(found[k], 0)
            valid = found[k] >= 0
            start = pl.multiple_of(b * LANES, LANES)
            live = lane < jnp.where(valid, block_count_ref[b], 0)
            named = lane == jnp.where(valid, leaf_ref[b], -1)
            star_send[o, k, 0:3] = star_pos_ref[:, pl.ds(start, LANES)]
            star_send[o, k, 3:4] = jnp.where(live, energy_ref[pl.ds(b, 1), :], 0.0)
            star_send[o, k, 4:7] = jnp.where(live, star_mom_ref[:, pl.ds(start, LANES)], 0.0)
            star_send[o, k, 7:8] = jnp.where(named, 1.0, 0.0).astype(F32)


def kernel(
    sizes,
    own_ref, smooth_ref, ghost_send, star_send,
    accel_ref, deposit_ref,
    src, ghost_recv, star_recv,
    feat, side_a, side_b, weights, acc, table, marker, gathered, dep,
    ghost_ssem, ghost_rsem, star_ssem, star_rsem,
):
    n_x, n_y, n_z, leaves, ghosts, blocks = sizes
    owners = n_y * n_z
    rows = leaves * LANES
    wide = ghosts * LANES
    x, y, z = lax.axis_index("gx"), lax.axis_index("gy"), lax.axis_index("gz")
    me = y * n_z + z

    def owner_at(d):
        other = lax.rem(me + d, owners)
        return other, (x, lax.div(other, n_z), lax.rem(other, n_z))

    def beside(k):
        step = 1 if k % 2 == 0 else -1
        if k < 2:
            return (lax.rem(x + step + n_x, n_x), y, z)
        return (x, lax.rem(y + step + n_y, n_y), z)

    barrier = pltpu.get_barrier_semaphore()
    for k in range(2):
        pl.semaphore_signal(barrier, inc=1, device_id=beside(k), device_id_type=MESH)

    @pl.loop(1, owners)
    def _(d):
        pl.semaphore_signal(barrier, inc=1, device_id=owner_at(d)[1], device_id_type=MESH)

    src[:, 0:rows] = own_ref[...]
    pl.semaphore_wait(barrier, owners + 1)

    def ghost_copy(k):
        return pltpu.make_async_remote_copy(
            src_ref=ghost_send.at[k], dst_ref=ghost_recv.at[k],
            send_sem=ghost_ssem.at[k], recv_sem=ghost_rsem.at[k],
            device_id=beside(k), device_id_type=MESH,
        )

    def star_copy(d):
        other, where = owner_at(d)
        return pltpu.make_async_remote_copy(
            src_ref=star_send.at[other], dst_ref=star_recv.at[me],
            send_sem=star_ssem.at[d], recv_sem=star_rsem.at[d],
            device_id=where, device_id_type=MESH,
        )

    for k in range(4):
        ghost_copy(k).start()

    @pl.loop(1, owners)
    def _(d):
        star_copy(d).start()

    star_recv[me] = star_send[me]

    def put(rows_of):
        at = 0
        for piece in rows_of:
            feat[at : at + piece.shape[0], :] = piece
            at += piece.shape[0]
        if at < FEATURES:
            feat[at:FEATURES, :] = jnp.zeros((FEATURES - at, SOURCES), F32)

    def prepare(start, targets):
        here = pl.ds(start, SOURCES)
        u = src[0:3, here] - 0.5
        mass = src[3:4, here]
        norm = SCALE * jnp.sum(u * u, axis=0, keepdims=True)
        a = split3((-2.0 * SCALE) * u)
        n = split3(norm + SCALE * SOFT_SQ)
        one = jnp.ones((1, SOURCES), F32)
        put([a[0]] * 3 + [a[1]] * 3 + [a[2]] * 3 + list(n) + [one] * 3)
        side_a[here, :] = feat[...].T.astype(BF16)
        wx, wm = split3(mass * u), split3(mass)
        put([wx[0], wm[0], wx[1], wm[1], wx[2], wm[2]])
        weights[:, here] = feat[0:16, :].astype(BF16)
        if targets:
            b = split3(u)
            put(list(b) * 3 + [one] * 3 + list(split3(norm)))
            side_b[:, here] = feat[...].astype(BF16)

    @pl.loop(0, rows // SOURCES)
    def _(c):
        prepare(pl.multiple_of(c * SOURCES, SOURCES), True)

    def pairs(start, right):
        d = jnp.dot(
            side_a[pl.ds(start, SOURCES), :], right, preferred_element_type=F32
        )
        value = jnp.exp2(-1.5 * (d + lax.log2(d)))
        high = value.astype(BF16)
        low = (value - high.astype(F32)).astype(BF16)
        w = weights[:, pl.ds(start, SOURCES)]
        return jnp.dot(w, high, preferred_element_type=F32) + jnp.dot(
            w, low, preferred_element_type=F32
        )

    def over(first, count, right, total, unroll):
        def step(c, total):
            start = pl.multiple_of(first + c * SOURCES, SOURCES)
            return total + pairs(start, right)

        return lax.fori_loop(0, count, step, total, unroll=unroll)

    @pl.loop(0, rows // TARGETS)
    def _(t):
        here = pl.ds(pl.multiple_of(t * TARGETS, TARGETS), TARGETS)
        acc[:, here] = over(
            0, rows // SOURCES, side_b[:, here], jnp.zeros((16, TARGETS), F32), UNROLL
        )

    for k in range(4):
        ghost_copy(k).wait()
        there = slice(rows + k * wide, rows + (k + 1) * wide)
        src[:, there] = ghost_recv[k]
        shifted = slice(k // 2, k // 2 + 1)
        src[shifted, there] = src[shifted, there] + (-1.0 if k % 2 == 0 else 1.0)

    @pl.loop(0, 4 * wide // SOURCES)
    def _(c):
        prepare(pl.multiple_of(rows + c * SOURCES, SOURCES), False)

    @pl.loop(0, rows // TARGETS)
    def _(t):
        here = pl.ds(pl.multiple_of(t * TARGETS, TARGETS), TARGETS)
        total = over(rows, 4 * wide // SOURCES, side_b[:, here], acc[:, here], True)
        total = total[0:4] + total[4:8] + total[8:12]
        u = src[0:3, here] - 0.5
        value = FACTOR * (total[0:3] - u * total[3:4])
        accel_ref[:, here] = jnp.where(src[4:5, here] > 0.5, value, 0.0)

    h = smooth_ref[...]
    table[:, 3 * LANES :] = 1.0 / (h * h)
    for l in range(leaves):
        for c in range(3):
            table[l : l + 1, c * LANES : (c + 1) * LANES] = src[
                c : c + 1, l * LANES : (l + 1) * LANES
            ]

    @pl.loop(1, owners)
    def _(d):
        star_copy(d).wait()

    @pl.loop(0, owners)
    def _(o):
        for k in range(SLOTS):
            marker[pl.ds(o * SLOTS + k, 1), :] = star_recv[o, k, 7:8]

    for c in range(4):
        gathered[c] = jnp.dot(
            marker[:, 0:leaves],
            table[:, c * LANES : (c + 1) * LANES],
            precision=HIGHEST,
            preferred_element_type=F32,
        )

    @pl.loop(0, owners)
    def _(o):
        for k in range(SLOTS):
            at = pl.ds(o * SLOTS + k, 1)
            star = star_recv[o, k].T
            gas = [gathered[c, at, :] for c in range(4)]
            seps = [gas[c] - star[:, c : c + 1] for c in range(3)]
            distance = seps[0] * seps[0] + seps[1] * seps[1] + seps[2] * seps[2]
            weight = jnp.exp(-distance * gas[3])
            share = weight / (1.0 + jnp.sum(weight, axis=1, keepdims=True))
            heat = star[:, 3:4] * share
            dep[0, at, :] = jnp.sum(heat, axis=0, keepdims=True)
            for c in range(3):
                kick = share * star[:, 4 + c : 5 + c] + RADIAL_PUSH * heat * seps[c]
                dep[c + 1, at, :] = jnp.sum(kick, axis=0, keepdims=True)

    named = marker[...].T[0:leaves]
    for c in range(4):
        table[:, c * LANES : (c + 1) * LANES] = jnp.dot(
            named, dep[c], precision=HIGHEST, preferred_element_type=F32
        )
    for l in range(leaves):
        alive = src[4:5, l * LANES : (l + 1) * LANES] > 0.5
        for c in range(4):
            deposit_ref[c : c + 1, l * LANES : (l + 1) * LANES] = jnp.where(
                alive, table[l : l + 1, c * LANES : (c + 1) * LANES], 0.0
            )


def on_device(
    mesh_sizes,
    gas_position, gas_mass, gas_smoothing, leaf_counts, ghost_lists,
    star_position, star_energy, star_momentum, block_counts, block_owners, block_leaves,
):
    n_x, n_y, n_z = mesh_sizes
    leaves = leaf_counts.shape[0]
    blocks = block_counts.shape[0]
    ghosts = ghost_lists.shape[2]
    rows = leaves * LANES
    owners = n_y * n_z
    slots = owners * SLOTS
    slot_rows = -(-slots // 8) * 8
    total = rows + 4 * ghosts * LANES
    vmem = pl.BlockSpec(memory_space=pltpu.VMEM)
    smem = pl.BlockSpec(memory_space=pltpu.SMEM)
    sizes = (n_x, n_y, n_z, leaves, ghosts, blocks)
    own, ghost_send, star_send = pl.pallas_call(
        functools.partial(prepare_sends, sizes),
        out_shape=(
            jax.ShapeDtypeStruct((8, rows), F32),
            jax.ShapeDtypeStruct((4, 8, ghosts * LANES), F32),
            jax.ShapeDtypeStruct((owners, SLOTS, 8, LANES), F32),
        ),
        in_specs=[vmem, vmem, smem, smem, vmem, vmem, vmem, smem, smem, smem],
        out_specs=(vmem, vmem, vmem),
    )(
        gas_position,
        gas_mass.reshape(leaves, LANES),
        leaf_counts,
        ghost_lists.reshape(-1),
        star_position,
        star_energy.reshape(blocks, LANES),
        star_momentum,
        block_counts,
        block_owners.reshape(-1),
        block_leaves,
    )
    return pl.pallas_call(
        functools.partial(kernel, sizes),
        out_shape=(
            jax.ShapeDtypeStruct((3, rows), F32),
            jax.ShapeDtypeStruct((4, rows), F32),
        ),
        in_specs=[vmem, vmem, vmem, vmem],
        out_specs=(vmem, vmem),
        scratch_shapes=[
            pltpu.VMEM((8, total), F32),
            pltpu.VMEM((4, 8, ghosts * LANES), F32),
            pltpu.VMEM((owners, SLOTS, 8, LANES), F32),
            pltpu.VMEM((FEATURES, SOURCES), F32),
            pltpu.VMEM((total, FEATURES), BF16),
            pltpu.VMEM((FEATURES, rows), BF16),
            pltpu.VMEM((16, total), BF16),
            pltpu.VMEM((16, rows), F32),
            pltpu.VMEM((leaves, 4 * LANES), F32),
            pltpu.VMEM((slot_rows, LANES), F32),
            pltpu.VMEM((4, slot_rows, LANES), F32),
            pltpu.VMEM((4, slot_rows, LANES), F32),
            pltpu.SemaphoreType.DMA((4,)),
            pltpu.SemaphoreType.DMA((4,)),
            pltpu.SemaphoreType.DMA((owners,)),
            pltpu.SemaphoreType.DMA((owners,)),
        ],
        compiler_params=pltpu.CompilerParams(collective_id=0, has_side_effects=True),
    )(own, gas_smoothing.reshape(leaves, LANES), ghost_send, star_send)


def solution(mesh):
    split = ("gx", "gy", "gz")
    placed = (
        P(None, split), P(split), P(split), P(split), P(split, None, None),
        P(None, split), P(split), P(None, split), P(split), P(split, None), P(split),
    )
    sizes = tuple(mesh.shape[axis] for axis in split)
    return jax.shard_map(
        functools.partial(on_device, sizes),
        mesh=mesh,
        in_specs=placed,
        out_specs=(P(None, split), P(None, split)),
        check_vma=False,
    )
```
